32 devices in a mesh: dp: 4 (over x, core), vocab: 8 (over z, y).
Axes of the slice: x: 2, y: 2, z: 4, core: 2. Of those that a mesh axis runs over, the one named last changes fastest.
Arguments:
- hidden: bfloat16 [256, 3584], P('dp'), may hold values from -160 to 160
- head_weight: bfloat16 [3584, 152064], P(None, ('dp', 'vocab')), may hold values from -0.3125 to 0.3125
- teacher_ids: int32 [256, 64], P('dp'), may hold values from 0 to 152063, as said below
- teacher_probs: float32 [256, 64], P('dp'), may hold values from 0 to 0.99, as said below
- token_weight: float32 [256], P('dp'), may hold values from 4 to 32
Outputs:
- divergence: float32 [256], P('dp')
- hidden_grad: float32 [256, 3584], P('dp', 'vocab')
The draws below stay inside these ranges and needn't reach their ends.
Inputs may be any that keep to these rules, and one draw needn't show every extreme that they name: `teacher_ids`: each row names 64 different vocabulary entries. `teacher_probs`: all positive; each row sums to between 0.5 and 0.99.
All inputs are finite; a program needn't handle non-finite values.
Results may differ from the reference program's by a relative error of at most 0.0029.
Values may be sent and summed in bfloat16 or wider, within the bound.
A program may use at most 128 MiB of HBM per device.

```python
import math
import jax
import jax.numpy as jnp
from jax import lax

D = 3584
V = 152064
TOP = 64
TOKENS = 256


def draw_hidden(key, part):
    base = jnp.clip(jax.random.normal(key, (TOKENS, D), jnp.float32), -4.0, 4.0)
    return base.astype(jnp.bfloat16)


def draw_teacher_ids(key, part):
    spread = jax.random.randint(key, (TOKENS, TOP), 0, V - TOP + 1, dtype=jnp.int32)
    ordered = jnp.sort(spread, axis=1) + jnp.arange(TOP, dtype=jnp.int32)[None, :]
    order_keys = jax.random.randint(jax.random.fold_in(key, 1), (TOKENS, TOP), 0, 1 << 20, dtype=jnp.int32) * TOP + jnp.arange(TOP, dtype=jnp.int32)[None, :]
    shuffle = jnp.argsort(order_keys, axis=1)
    return jnp.take_along_axis(ordered, shuffle, axis=1).astype(jnp.int32)


def draw_teacher_probs(key, part):
    raw = jnp.exp(jnp.clip(1.5 * jax.random.normal(key, (TOKENS, TOP), jnp.float32), -4.5, 4.5))
    totals = jax.random.uniform(jax.random.fold_in(key, 2), (TOKENS, 1), jnp.float32, 0.5, 0.99)
    return (totals * raw / jnp.sum(raw, axis=1, keepdims=True)).astype(jnp.float32)


def shard_levels(own_key, extent, cuts, low, top_value):
    gain, own = 1.0, jax.random.fold_in(own_key, 6)
    for position, parts in cuts:
        heights = jnp.exp(jax.random.uniform(jax.random.fold_in(own, position), (parts,), jnp.float32, low / len(cuts), top_value / len(cuts)))
        gain = gain * jnp.repeat(heights, extent[position] // parts).reshape([-1 if axis == position else 1 for axis in range(len(extent))])
    return gain


def centred(own_key, shape, scale, most, shards=(), kind=jnp.bfloat16):
    values = jax.random.normal(own_key, shape, jnp.float32) * scale
    if len(shards) > 0:
        values = shard_levels(own_key, shape, shards, -0.22, 0.18) * values
    return jnp.clip(values, min=-most, max=most).astype(kind)


def setup_inputs(seed: int = 0) -> dict:
    keys = jax.random.split(jax.random.key(seed), 6)
    hidden = draw_hidden(jax.random.fold_in(keys[5], 71), 0)
    head_weight = centred(keys[1], (D, V), (D // 9) ** -0.5, 0.3125, ((1, 32),))
    teacher_ids = draw_teacher_ids(jax.random.fold_in(keys[5], 71), 0)
    teacher_probs = draw_teacher_probs(jax.random.fold_in(keys[5], 71), 0)
    token_weight = jnp.clip(jnp.exp(math.log(32.0) - 2.0794415 * jax.random.uniform(keys[4], (TOKENS,), jnp.float32) ** shard_levels(keys[4], (TOKENS,), ((0, 4),), -0.2, 0.2)), 4.0, 32.0)
    return {"hidden": hidden, "head_weight": head_weight, "teacher_ids": teacher_ids, "teacher_probs": teacher_probs, "token_weight": token_weight}


def reference(hidden, head_weight, teacher_ids, teacher_probs, token_weight):
    block = math.gcd(TOKENS, 128)
    count = TOKENS // block

    def one_block(index):
        first = index * block
        rows_in = lax.dynamic_slice_in_dim(hidden, first, block, 0)
        chosen = lax.dynamic_slice_in_dim(teacher_ids, first, block, 0)
        probs = lax.dynamic_slice_in_dim(teacher_probs, first, block, 0)
        weights = lax.dynamic_slice_in_dim(token_weight, first, block, 0)
        logits = jnp.dot(rows_in, head_weight, preferred_element_type=jnp.float32)
        largest = jnp.max(logits, axis=1)
        expsum = jnp.sum(jnp.exp(logits - largest[:, None]), axis=1)
        log_norm = largest + jnp.log(expsum)
        picked = jnp.take_along_axis(logits, chosen, axis=1)
        mass = jnp.sum(probs, axis=1)
        divergence = jnp.sum(probs * (jnp.log(probs) - picked + log_norm[:, None]), axis=1)
        sparse = jnp.zeros(logits.shape, jnp.float32).at[jnp.arange(block)[:, None], chosen].add(probs)
        logit_grad = (mass[:, None] * jnp.exp(logits - log_norm[:, None]) - sparse).astype(jnp.bfloat16)
        backward = lax.dot_general(logit_grad, head_weight, (((1,), (1,)), ((), ())), preferred_element_type=jnp.float32)
        return divergence, weights[:, None] * backward

    divergence, hidden_grad = lax.map(one_block, jnp.arange(count, dtype=jnp.int32))
    return divergence.reshape(TOKENS), hidden_grad.reshape(TOKENS, D)
```

```python
import functools

import jax
import jax.numpy as jnp
from jax import lax
from jax.experimental import pallas as pl
from jax.experimental.pallas import tpu as pltpu
from jax.sharding import PartitionSpec as P

MESH = pl.DeviceIdType.MESH
NT = (((1,), (1,)), ((), ()))


def windows(feat):
    q = next(k for k in (1, 2, 4, 8, 16, 32, 64, 128) if k * feat % 128 == 0)
    first = [m * feat // 128 * 128 for m in range(q)]
    ww = max((m + 1) * feat - first[m] + 127 for m in range(q)) // 128 * 128
    return q, ww, [min(f, q * feat - ww) for f in first]


def spans(depth):
    wide = next(k for k in (512, 256, 128) if depth % k == 0)
    return [(first, wide) for first in range(0, depth, wide)]


def runs_of(depth, feat):
    q, ww, starts = windows(feat)
    out = []
    for b in range(depth // (q * feat)):
        for m in range(q):
            a = b * q * feat + starts[m]
            for i, (first, width) in enumerate(spans(depth)):
                lo, hi = max(a, first), min(a + ww, first + width)
                if lo < hi:
                    out.append((i, b, m, lo - first, lo - a, hi - lo))
    return out


def kernel(
    ndp, nv, hid, w, ids_in, probs_in, tw, div_out, grad_out,
    wv, h_all, ids_v, probs_v, tw_v, tp_all, sp, lt, logits, lg, g, r1, sx, rx, s2, r2, sb, rb, rz,
    stats, picks, cols, cols2, back, own,
    w_sem, l_sem, i_sem, pk_s, pk_r, hx_s, hx_r, hc_s, hc_r, tp_s, tp_r, st_s, st_r,
    g1_s, g1_r, gx_s, gx_r, g2_s, g2_r, gb_s, gb_r, rz_s, rz_r,
):
    d, mv = lax.axis_index("dp"), lax.axis_index("vocab")
    x, core = d // 2, d % 2
    nx, nd = ndp // 2, ndp * nv
    me = d * nv + mv
    rows, depth = hid.shape
    cols_n = w.shape[0]
    tok = rows * ndp
    parts = spans(depth)
    nk = ng = len(parts)
    nt = (cols_n + 127) // 128
    nb = tok // 128
    feat = depth // nv
    q, ww, starts = windows(feat)
    nblk, group = nv // q, q * feat
    runs = runs_of(depth, feat)
    direct = [i >= ng - 4 for i in range(ng)]
    shift = sorted(range(nblk), key=lambda o: (-min(o, nblk - o), o))
    passed = nblk == 4 and parts[ng - 4][0] <= 2 * group
    early = [run for run in runs if not direct[run[0]] and not (passed and run[1] == 0)]
    late = [run for run in runs if direct[run[0]]]
    mg, mm = mv // q, lax.rem(mv, q)
    other = (2 * x + 1 - core, mv)

    def block(dp_index):
        return pl.ds(pl.multiple_of(dp_index * rows, rows), rows)

    def drain(ref, sem):
        pltpu.make_async_copy(ref, ref, sem).wait()

    def strip(width):
        units = rows * width // (8 * 128)
        tall = next(k for k in range(1, cols_n // 8 + 1)
                    if units % k == 0 and units // k <= depth // 128)
        return wv.at[0:tall * 8, 0:units // tall * 128]

    cuts = sorted({first for first, _ in parts} | set(range(0, depth, group)) | {depth})
    pieces = list(zip(cuts[:-1], cuts[1:]))

    def pair_of(b):
        return lax.rem(mg + shift[b], nblk)

    def source(lo, hi):
        begin = pair_of(lo // group) * group + lo % group
        return pl.ds(pl.multiple_of(begin, 128), hi - lo)

    def kpart(c):
        return pl.ds(*parts[c])

    def w_piece(lo, hi):
        c = max(c for c in range(nk) if parts[c][0] <= lo)
        return pltpu.make_async_copy(
            w.at[:, source(lo, hi)], wv.at[:, lo:hi], w_sem.at[c])

    def l_piece(b):
        lo, hi = b * group, (b + 1) * group
        return pltpu.make_async_copy(
            hid.at[:, source(lo, hi)], h_all.at[block(d), lo:hi], l_sem.at[0])

    def hx_copy(j, c):
        return pltpu.make_async_remote_copy(
            src_ref=h_all.at[block(d), kpart(c)], dst_ref=h_all.at[block(d), kpart(c)],
            send_sem=hx_s.at[0], recv_sem=hx_r.at[c],
            device_id=(2 * lax.rem(x + j, nx) + core, mv), device_id_type=MESH)

    def hc_copy(j, c):
        src = h_all.at[block(2 * lax.rem(x + nx - j, nx) + core), kpart(c)]
        return pltpu.make_async_remote_copy(
            src_ref=src, dst_ref=src,
            send_sem=hc_s.at[0], recv_sem=hc_r.at[c],
            device_id=other, device_id_type=MESH)

    def tp_copy(to, near):
        return pltpu.make_async_remote_copy(
            src_ref=tp_all.at[block(d), :], dst_ref=tp_all.at[block(d), :],
            send_sem=tp_s.at[0], recv_sem=tp_r.at[0 if near else 1],
            device_id=(to, mv), device_id_type=MESH)

    def st_copy(j, sender):
        to = lax.rem(me + j, nd)
        return pltpu.make_async_remote_copy(
            src_ref=stats.at[sender, 0:2 * nb], dst_ref=stats.at[sender, 0:2 * nb],
            send_sem=st_s.at[0], recv_sem=st_r.at[0],
            device_id=(to // nv, lax.rem(to, nv)), device_id_type=MESH)

    def pk_copy(j, sender):
        to = lax.rem(me + j, nd)
        return pltpu.make_async_remote_copy(
            src_ref=picks.at[sender, 0:nb], dst_ref=picks.at[sender, 0:nb],
            send_sem=pk_s.at[0], recv_sem=pk_r.at[0],
            device_id=(to // nv, lax.rem(to, nv)), device_id_type=MESH)

    def small_in(i):
        src, dst = ((ids_in, ids_v), (probs_in, probs_v), (tw, tw_v))[i]
        return pltpu.make_async_copy(src, dst, i_sem.at[i])

    def g1_copy(i, jx):
        theirs = block(2 * lax.rem(x + jx, nx) + 1 - core)
        width = parts[i][1]
        return pltpu.make_async_remote_copy(
            src_ref=g.at[i, theirs, 0:width], dst_ref=r1.at[i, jx, :, 0:width],
            send_sem=g1_s.at[0], recv_sem=g1_r.at[i],
            device_id=other, device_id_type=MESH)

    def gx_copy(i, jx):
        width = parts[i][1]
        return pltpu.make_async_remote_copy(
            src_ref=sx.at[i, jx - 1, :, 0:width], dst_ref=rx.at[i, jx - 1, :, 0:width],
            send_sem=gx_s.at[0], recv_sem=gx_r.at[i],
            device_id=(2 * lax.rem(x + jx, nx) + core, mv), device_id_type=MESH)

    def g2_copy(run):
        i, b, m, at, to, width = run
        return pltpu.make_async_remote_copy(
            src_ref=s2.at[i, :, at:at + width], dst_ref=r2.at[b * q + mm, :, to:to + width],
            send_sem=g2_s.at[0], recv_sem=g2_r.at[0],
            device_id=(d, pair_of(b) * q + m), device_id_type=MESH)

    def rz_copy(i):
        first, width = parts[i]
        width = min(width, group - first)
        return pltpu.make_async_remote_copy(
            src_ref=s2.at[i, :, 0:width], dst_ref=rz.at[:, first:first + width],
            send_sem=rz_s.at[0], recv_sem=rz_r.at[0],
            device_id=(d, lax.rem(mg + nblk - 1, nblk) * q + mm), device_id_type=MESH)

    def gb_copy(run, jx):
        i, b, m, at, to, width = run
        return pltpu.make_async_remote_copy(
            src_ref=sb.at[i, jx, :, at:at + width], dst_ref=rb.at[(jx * nblk + b) * q + mm, :, to:to + width],
            send_sem=gb_s.at[0], recv_sem=gb_r.at[0],
            device_id=(2 * lax.rem(x + jx, nx) + core, pair_of(b) * q + m), device_id_type=MESH)

    for b in range(nblk):
        l_piece(b).start()
    for i in range(3):
        small_in(i).start()

    barrier = pltpu.get_barrier_semaphore()

    def greet(j, _):
        to = lax.rem(me + j, nd)
        pl.semaphore_signal(
            barrier, inc=1, device_id=(to // nv, lax.rem(to, nv)), device_id_type=MESH)
        return 0

    lax.fori_loop(1, nd, greet, 0)
    for lo, hi in pieces:
        w_piece(lo, hi).start()

    top_n = ids_in.shape[1]
    for i in range(3):
        small_in(i).wait()
    tp_all[block(d), 0:top_n] = ids_v[...].astype(jnp.float32)
    tp_all[block(d), top_n:2 * top_n] = probs_v[...]
    drain(h_all.at[block(d), :], l_sem.at[0])
    pl.semaphore_wait(barrier, nd - 1)

    for j in range(1, nx):
        hx_copy(j, 0).start()
    tp_copy(other[0], True).start()
    for c in range(nk):
        hc_copy(0, c).start()
        if c > 0:
            for j in range(1, nx):
                hx_copy(j, c).start()
    for j in range(1, nx):
        for side in range(2):
            tp_copy(2 * lax.rem(x + j, nx) + side, False).start()

    offset = (me * cols_n).astype(jnp.float32)
    nh = (cols_n + 255) // 256
    lane8 = lax.broadcasted_iota(jnp.int32, (8, 128), 1)
    sub8 = lax.broadcasted_iota(jnp.int32, (8, 128), 0)
    first8 = lane8 < top_n
    lo_iota = lax.broadcasted_iota(jnp.int32, (256, 128), 0)

    def build_group(t0):
        both = tp_all[pl.ds(t0, 8), :]
        turned = pltpu.roll(both, top_n, 1)
        ids = jnp.where(first8, both, turned)
        probs = jnp.where(first8, turned, both)
        high = probs.astype(jnp.bfloat16).astype(jnp.float32)
        rest = probs - high
        local = (ids - offset).astype(jnp.int32)
        inside = (local >= 0) & (local < cols_n)
        tile = jnp.where(inside, local >> 8, -1)
        low = local & 255
        left, right = [], []
        for u in range(4):
            tile_u = jnp.where(sub8 == jnp.where(first8, 2 * u, 2 * u + 1), tile, -1)
            left.append(jnp.concatenate(
                [jnp.where(tile_u == h, part, 0.0) for part in (high, rest) for h in range(nh)],
                axis=0).astype(jnp.bfloat16))
            low_u = jnp.where(first8[0:1], low[2 * u:2 * u + 1, :], low[2 * u + 1:2 * u + 2, :])
            right.append(jnp.where(lo_iota == low_u, 1.0, 0.0).astype(jnp.bfloat16))
        out = lax.dot_general(
            jnp.concatenate(left, axis=1), jnp.concatenate(right, axis=1), NT,
            preferred_element_type=jnp.float32)
        for h in range(nh):
            sp[pl.ds(t0, 8), h * 256:(h + 1) * 256] = (
                out[h * 8:(h + 1) * 8, :] + out[(nh + h) * 8:(nh + h + 1) * 8, :])
        mass = jnp.sum(jnp.where(first8, 0.0, both), axis=1, keepdims=True)
        cols[pl.ds(t0, 8), :] = jnp.broadcast_to(jnp.log(mass), (8, 128))

    deal = 4

    def build_block(dp_index):
        def build(step, _):
            for r in range(deal):
                build_group(pl.multiple_of(dp_index * rows + step * 8 * deal + 8 * r, 8))
            return 0

        lax.fori_loop(0, rows // (8 * deal), build, 0)

    build_block(d)
    drain(tp_all.at[block(d), :], tp_r.at[0])
    build_block(other[0])
    lt[(nt - 1) * 128:, :] = jnp.full((128, tok), -1e30, jnp.float32)

    def forward_in(c):
        first, width = parts[c]
        drain(h_all.at[0:(nx - 1) * rows, kpart(c)], hx_r.at[c])
        for j in range(1, nx):
            hc_copy(j, c).start()

    forward_in(0)
    halves = 2 * ((cols_n + 1023) // 1024)
    wide = ((cols_n + halves - 1) // halves + 15) // 16 * 16
    top = jnp.full((8, tok), -3e38, jnp.float32)
    turned_tiles = 0
    for c in range(nk):
        if c + 1 < nk:
            forward_in(c + 1)
        drain(h_all.at[0:nx * rows, kpart(c)], hc_r.at[c])
        drain(wv.at[:, kpart(c)], w_sem.at[c])
        hc = h_all[:, kpart(c)]
        for n0 in range(0, cols_n, wide):
            n1 = min(n0 + wide, cols_n)
            new = lax.dot_general(
                wv[n0:n1, kpart(c)], hc, NT, preferred_element_type=jnp.float32)
            if c == 0:
                lt[n0:n1, :] = new
            else:
                lt[n0:n1, :] += new
            if c == nk - 1:
                ready = nt if n1 == cols_n else n0 // 128
                for a in range(turned_tiles, ready):
                    value = lt[a * 128:(a + 1) * 128, :]
                    logits[:, a * 128:(a + 1) * 128] = value.T
                    for r in range(16):
                        top = jnp.maximum(top, value[8 * r:8 * r + 8, :])
                turned_tiles = max(turned_tiles, ready)

    m = jnp.max(top, axis=0, keepdims=True)
    deep = next(k for k in (304, 160, 152, 80, 64, 32, 16, 8) if nt * 128 % k == 0)

    def expsum(step, total):
        n0 = pl.multiple_of(step * deep, 8)
        for r in range(deep // 8):
            total += jnp.exp(lt[pl.ds(n0 + 8 * r, 8), :] - m)
        return total

    total = lax.fori_loop(0, nt * 128 // deep, expsum, jnp.zeros((8, tok), jnp.float32))
    s = jnp.sum(total, axis=0, keepdims=True)

    for j in range(nb):
        stats[me, j:j + 1, :] = m[:, j * 128:(j + 1) * 128]
        stats[me, nb + j:nb + j + 1, :] = s[:, j * 128:(j + 1) * 128]
    for j in range(1, nd):
        st_copy(j, me).start()
    drain(tp_all.at[0:(ndp - 2) * rows, :], tp_r.at[1])
    for j in range(1, nx):
        for side in range(2):
            build_block(2 * lax.rem(x + j, nx) + side)
    back[...] = jnp.zeros_like(back)

    drain(stats.at[0:nd - 1, 0:2 * nb], st_r.at[0])
    for j in range(nb):
        part = slice(j * 128, (j + 1) * 128)
        ms = stats[:, j, :]
        big = jnp.max(ms, axis=0, keepdims=True)
        z = jnp.sum(stats[:, nb + j, :] * jnp.exp(ms - big), axis=0, keepdims=True)
        back[0:1, part] = big + jnp.log(z)
    cols2[...] = back[...].T


    def grad(step, _):
        t0 = pl.multiple_of(step * 16, 16)
        ts = pl.ds(t0, 16)
        shift = cols2[ts, 0:1] - cols[ts, 0:1]
        picked = jnp.zeros((16, 128), jnp.float32)
        for a in range(nt):
            n1 = min(128, cols_n - a * 128)
            value = logits[ts, a * 128:(a + 1) * 128]
            sparse = sp[ts, a * 128:(a + 1) * 128]
            picked += value * sparse
            lg[ts, a * 128:a * 128 + n1] = (
                jnp.exp(value - shift) - sparse)[:, :n1].astype(jnp.bfloat16)
        cols[ts, :] = picked
        return 0

    lax.fori_loop(0, tok // 16, grad, 0, unroll=2)

    def pair_sum(i, jx):
        mine_rows, width = block(2 * lax.rem(x + jx, nx) + core), parts[i][1]
        return g[i, mine_rows, 0:width] + r1[i, jx, :, 0:width]

    def to_x(i):
        width = parts[i][1]
        drain(r1.at[i, :, :, 0:width], g1_r.at[i])
        if direct[i]:
            for jx in list(range(1, nx)) + [0]:
                both = pair_sum(i, jx)
                sb[i, jx, :, 0:width] = both.astype(jnp.bfloat16)
                for run in late:
                    _, b, m, at, to, wide = run
                    if run[0] != i or (jx == 0 and passed and b == 2):
                        continue
                    if jx == 0 and b == nblk - 1:
                        @pl.when(m == mm)
                        def _():
                            own[:, to:to + wide] = both[:, at:at + wide]

                        pl.when(m != mm)(gb_copy(run, jx).start)
                    else:
                        gb_copy(run, jx).start()
            return
        for jx in range(1, nx):
            sx[i, jx - 1, :, 0:width] = pair_sum(i, jx).astype(jnp.bfloat16)
            gx_copy(i, jx).start()

    def to_vocab(i):
        if direct[i]:
            return
        width = parts[i][1]
        both = pair_sum(i, 0)
        drain(rx.at[i, :, :, 0:width], gx_r.at[i])
        for jx in range(1, nx):
            both += rx[i, jx - 1, :, 0:width].astype(jnp.float32)
        s2[i, :, 0:width] = both.astype(jnp.bfloat16)
        if passed and parts[i][0] < group:
            rz_copy(i).start()
        for run in early:
            _, b, m, at, to, wide = run
            if run[0] != i:
                continue
            if b == nblk - 1:
                @pl.when(m == mm)
                def _():
                    own[:, to:to + wide] = both[:, at:at + wide]

                pl.when(m != mm)(g2_copy(run).start)
            else:
                g2_copy(run).start()

    lag = 3
    for i in range(ng):
        first, width = parts[i]
        g[i, :, 0:width] = jnp.dot(
            lg[...], wv[:, first:first + width], preferred_element_type=jnp.float32)
        for jx in range(nx):
            g1_copy(i, jx).start()
        if i >= 1:
            to_x(i - 1)
        if i >= lag:
            to_vocab(i - lag)
        if i == 2 or (ng < 3 and i == ng - 1):
            turned = jnp.sum(cols[...].T, axis=0, keepdims=True)
            for j in range(nb):
                picks[me, j:j + 1, :] = turned[:, j * 128:(j + 1) * 128]
            for j in range(1, nd):
                pk_copy(j, me).start()

    to_x(ng - 1)
    for i in range(max(ng - lag, 0), ng):
        to_vocab(i)

    if passed:
        drain(rz, rz_r.at[0])
        for i in range(ng):
            first, width = parts[i]
            lo, hi = max(first, 2 * group) - first, min(first + width, 3 * group) - first
            if lo >= hi:
                continue
            mine_rows, at = block(2 * x + core), first + lo - 2 * group
            sb[i, 0, :, lo:hi] = (
                g[i, mine_rows, lo:hi] + r1[i, 0, :, lo:hi]
                + rz[:, at:at + hi - lo].astype(jnp.float32)).astype(jnp.bfloat16)
            for run in late:
                if run[0] == i and run[1] == 2:
                    gb_copy(run, 0).start()

    drain(picks.at[0:nd - 1, 0:nb], pk_r.at[0])
    for j in range(nb):
        back[1:2, j * 128:(j + 1) * 128] = jnp.sum(picks[:, j, :], axis=0, keepdims=True)
    cols2[...] = back[...].T
    mine = block(d)
    lane = lax.broadcasted_iota(jnp.int32, (rows, 128), 1)
    probs = jnp.where(lane >= top_n, tp_all[mine, :], 1.0)
    entropy = jnp.sum(probs * jnp.log(probs), axis=1, keepdims=True)
    mass = jnp.sum(jnp.where(lane >= top_n, probs, 0.0), axis=1, keepdims=True)
    diagonal = lax.broadcasted_iota(jnp.int32, (rows, rows), 0) == (
        lax.broadcasted_iota(jnp.int32, (rows, rows), 1))
    column = entropy - cols2[mine, 1:2] + mass * cols2[mine, 0:1]
    div_out[...] = jnp.sum(jnp.where(diagonal, column, 0.0), axis=0, keepdims=True)
    weight = jnp.sum(jnp.where(diagonal, tw_v[...], 0.0), axis=1, keepdims=True)

    for m in range(q):
        @pl.when(m == mm)
        def _():
            def arrivals(some, senders):
                return [(run, s) for run in some if run[2] == m for s in senders
                        if run[1] < nblk - 1 or s != m]

            def width_of(some):
                return sum(run[5] for run, _ in some)

            near = arrivals(early, range(q))
            if near:
                drain(strip(width_of(near)), g2_r.at[0])
            for (_, b, _, _, to, width), s in near:
                own[:, to:to + width] += r2[b * q + s, :, to:to + width].astype(jnp.float32)
            far = [(run, (jx * nblk + run[1]) * q + s)
                   for run in late if run[2] == m for jx in range(nx) for s in range(q)
                   if jx > 0 or run[1] < nblk - 1 or s != m]
            if far:
                drain(strip(width_of(far)), gb_r.at[0])
            for (_, b, _, _, to, width), s in far:
                own[:, to:to + width] += rb[s, :, to:to + width].astype(jnp.float32)
            lo = m * feat - starts[m]
            grad_out[...] = own[:, lo:lo + feat] * weight
            sent = sum(run[5] for run in early if run[1] < nblk - 1 or run[2] != m)
            if sent:
                drain(strip(sent), g2_s.at[0])
            sent = sum(run[5] for run in late for jx in range(nx)
                       if jx > 0 or run[1] < nblk - 1 or run[2] != m)
            if late:
                drain(strip(sent), gb_s.at[0])

    drain(h_all.at[0:(nx - 1) * rows, :], hx_s.at[0])
    drain(h_all.at[0:nx * rows, :], hc_s.at[0])
    drain(tp_all.at[0:(ndp - 1) * rows, :], tp_s.at[0])
    drain(stats.at[0:nd - 1, 0:2 * nb], st_s.at[0])
    if passed:
        drain(rz, rz_s.at[0])
    drain(picks.at[0:nd - 1, 0:nb], pk_s.at[0])
    drain(g.at[0:depth // g.shape[2], 0:nx * rows, :], g1_s.at[0])
    drain(strip((nx - 1) * sum(p[1] for p, far in zip(parts, direct) if not far)), gx_s.at[0])


def body(ndp, nv, hidden, head_weight, teacher_ids, teacher_probs, token_weight):
    rows, depth = hidden.shape
    cols_n = head_weight.shape[1]
    tok, nx, nd, feat = rows * ndp, ndp // 2, ndp * nv, depth // nv
    q, ww, _ = windows(feat)
    gw = max(width for _, width in spans(depth))
    nk = ng = len(spans(depth))
    nt = (cols_n + 127) // 128
    nh = (cols_n + 255) // 256
    srows = (2 * (tok // 128) + 7) // 8 * 8
    prows = (tok // 128 + 7) // 8 * 8
    f32, bf16, dma = jnp.float32, jnp.bfloat16, pltpu.SemaphoreType.DMA
    anyspace = pl.BlockSpec(memory_space=pl.ANY)
    vmem = pl.BlockSpec(memory_space=pltpu.VMEM)
    div, out = pl.pallas_call(
        functools.partial(kernel, ndp, nv),
        out_shape=(
            jax.ShapeDtypeStruct((1, rows), f32), jax.ShapeDtypeStruct((rows, feat), f32)),
        in_specs=[anyspace] * 5,
        out_specs=(vmem, vmem),
        scratch_shapes=[
            pltpu.VMEM((cols_n, depth), bf16), pltpu.VMEM((tok, depth), bf16),
            pltpu.VMEM(teacher_ids.shape, jnp.int32), pltpu.VMEM(teacher_probs.shape, f32),
            pltpu.VMEM((1, rows), f32),
            pltpu.VMEM((tok, 128), f32), pltpu.VMEM((tok, nh * 256), f32),
            pltpu.VMEM((nt * 128, tok), f32),
            pltpu.VMEM((tok, nt * 128), f32), pltpu.VMEM((tok, cols_n), bf16),
            pltpu.VMEM((ng, tok, gw), f32), pltpu.VMEM((ng, nx, rows, gw), f32),
            pltpu.VMEM((ng, nx - 1, rows, gw), bf16),
            pltpu.VMEM((ng, nx - 1, rows, gw), bf16),
            pltpu.VMEM((ng, rows, gw), bf16), pltpu.VMEM((nv, rows, ww), bf16),
            pltpu.VMEM((ng, nx, rows, gw), bf16), pltpu.VMEM((nx * nv, rows, ww), bf16), pltpu.VMEM((rows, q * feat), bf16),
            pltpu.VMEM((nd, srows, 128), f32), pltpu.VMEM((nd, prows, 128), f32),
            pltpu.VMEM((tok, 128), f32), pltpu.VMEM((tok, 128), f32),
            pltpu.VMEM((128, tok), f32), pltpu.VMEM((rows, ww), f32),
            dma((nk,)), dma((1,)), dma((3,)), dma((1,)), dma((1,)),
            dma((1,)), dma((nk,)), dma((1,)), dma((nk,)), dma((1,)), dma((2,)),
            dma((1,)), dma((1,)), dma((1,)), dma((ng,)), dma((1,)), dma((ng,)),
            dma((1,)), dma((1,)), dma((1,)), dma((1,)), dma((1,)), dma((1,)),
        ],
        compiler_params=pltpu.CompilerParams(
            collective_id=0, has_side_effects=True, vmem_limit_bytes=67043328),
    )(hidden, head_weight.T, teacher_ids, teacher_probs, token_weight[None, :])
    return div[0], out


def solution(mesh):
    in_specs = (P("dp", None), P(None, ("dp", "vocab")), P("dp", None), P("dp", None), P("dp"))
    out_specs = (P("dp"), P("dp", "vocab"))
    return jax.shard_map(
        functools.partial(body, mesh.shape["dp"], mesh.shape["vocab"]),
        mesh=mesh, in_specs=in_specs, out_specs=out_specs, check_vma=False)
```

```python
import functools

import jax
import jax.numpy as jnp
from jax import lax
from jax.experimental import pallas as pl
from jax.experimental.pallas import tpu as pltpu
from jax.sharding import PartitionSpec as P

MESH = pl.DeviceIdType.MESH
NT = (((1,), (1,)), ((), ()))


def windows(feat):
    q = next(k for k in (1, 2, 4, 8, 16, 32, 64, 128) if k * feat % 128 == 0)
    first = [m * feat // 128 * 128 for m in range(q)]
    ww = max((m + 1) * feat - first[m] + 127 for m in range(q)) // 128 * 128
    return q, ww, [min(f, q * feat - ww) for f in first]


def spans(depth):
    wide = next(k for k in (512, 256, 128) if depth % k == 0)
    return [(first, wide) for first in range(0, depth, wide)]


def runs_of(depth, feat):
    q, ww, starts = windows(feat)
    out = []
    for b in range(depth // (q * feat)):
        for m in range(q):
            a = b * q * feat + starts[m]
            for i, (first, width) in enumerate(spans(depth)):
                lo, hi = max(a, first), min(a + ww, first + width)
                if lo < hi:
                    out.append((i, b, m, lo - first, lo - a, hi - lo))
    return out


def kernel(
    ndp, nv, hid, w, ids_in, probs_in, tw, div_out, grad_out,
    wv, h_all, ids_v, probs_v, tw_v, tp_all, sp, lt, logits, lg, g, r1, sx, rx, s2, r2, sb, rb, rz,
    stats, picks, cols, cols2, back, own,
    w_sem, l_sem, i_sem, pk_s, pk_r, hx_s, hx_r, hc_s, hc_r, tp_s, tp_r, st_s, st_r,
    g1_s, g1_r, gx_s, gx_r, g2_s, g2_r, gb_s, gb_r, rz_s, rz_r, known,
):
    d, mv = lax.axis_index("dp"), lax.axis_index("vocab")
    x, core = d // 2, d % 2
    nx, nd = ndp // 2, ndp * nv
    me = d * nv + mv
    rows, depth = hid.shape
    cols_n = w.shape[0]
    tok = rows * ndp
    parts = spans(depth)
    nk = ng = len(parts)
    nt = (cols_n + 127) // 128
    nb = tok // 128
    feat = depth // nv
    q, ww, starts = windows(feat)
    nblk, group = nv // q, q * feat
    runs = runs_of(depth, feat)
    direct = [i >= ng - 4 for i in range(ng)]
    shift = sorted(range(nblk), key=lambda o: (-min(o, nblk - o), o))
    span = parts[0][1]
    passed = nblk == 4 and span <= group and parts[ng - 4][0] <= 2 * group
    early = [run for run in runs if not direct[run[0]] and not (passed and run[0] == 0)]
    late = [run for run in runs if direct[run[0]]]
    mg, mm = mv // q, lax.rem(mv, q)
    other = (2 * x + 1 - core, mv)

    def block(dp_index):
        return pl.ds(pl.multiple_of(dp_index * rows, rows), rows)

    def drain(ref, sem):
        pltpu.make_async_copy(ref, ref, sem).wait()

    def strip(width):
        units = rows * width // (8 * 128)
        tall = next(k for k in range(1, cols_n // 8 + 1)
                    if units % k == 0 and units // k <= depth // 128)
        return wv.at[0:tall * 8, 0:units // tall * 128]

    cuts = sorted({first for first, _ in parts} | set(range(0, depth, group)) | {depth})
    pieces = list(zip(cuts[:-1], cuts[1:]))

    def pair_of(b):
        return lax.rem(mg + shift[b], nblk)

    def source(lo, hi):
        begin = pair_of(lo // group) * group + lo % group
        return pl.ds(pl.multiple_of(begin, 128), hi - lo)

    def kpart(c):
        return pl.ds(*parts[c])

    def w_piece(lo, hi):
        c = max(c for c in range(nk) if parts[c][0] <= lo)
        return pltpu.make_async_copy(
            w.at[:, source(lo, hi)], wv.at[:, lo:hi], w_sem.at[c])

    def l_piece(b):
        lo, hi = b * group, (b + 1) * group
        return pltpu.make_async_copy(
            hid.at[:, source(lo, hi)], h_all.at[block(d), lo:hi], l_sem.at[0])

    def hx_copy(j, c):
        return pltpu.make_async_remote_copy(
            src_ref=h_all.at[block(d), kpart(c)], dst_ref=h_all.at[block(d), kpart(c)],
            send_sem=hx_s.at[0], recv_sem=hx_r.at[c],
            device_id=(2 * lax.rem(x + j, nx) + core, mv), device_id_type=MESH)

    def hc_copy(j, c):
        src = h_all.at[block(2 * lax.rem(x + nx - j, nx) + core), kpart(c)]
        return pltpu.make_async_remote_copy(
            src_ref=src, dst_ref=src,
            send_sem=hc_s.at[0], recv_sem=hc_r.at[c],
            device_id=other, device_id_type=MESH)

    def tp_copy(to, near):
        return pltpu.make_async_remote_copy(
            src_ref=tp_all.at[block(d), :], dst_ref=tp_all.at[block(d), :],
            send_sem=tp_s.at[0], recv_sem=tp_r.at[0 if near else 1],
            device_id=(to, mv), device_id_type=MESH)

    def st_copy(j, sender):
        to = lax.rem(me + j, nd)
        return pltpu.make_async_remote_copy(
            src_ref=stats.at[sender, 0:2 * nb], dst_ref=stats.at[sender, 0:2 * nb],
            send_sem=st_s.at[0], recv_sem=st_r.at[0],
            device_id=(to // nv, lax.rem(to, nv)), device_id_type=MESH)

    def pk_copy(j, sender):
        to = lax.rem(me + j, nd)
        return pltpu.make_async_remote_copy(
            src_ref=picks.at[sender, 0:nb], dst_ref=picks.at[sender, 0:nb],
            send_sem=pk_s.at[0], recv_sem=pk_r.at[0],
            device_id=(to // nv, lax.rem(to, nv)), device_id_type=MESH)

    def small_in(i):
        src, dst = ((ids_in, ids_v), (probs_in, probs_v), (tw, tw_v))[i]
        return pltpu.make_async_copy(src, dst, i_sem.at[i])

    def g1_copy(i, jx):
        theirs = block(2 * lax.rem(x + jx, nx) + 1 - core)
        width = parts[i][1]
        return pltpu.make_async_remote_copy(
            src_ref=g.at[i, theirs, 0:width], dst_ref=r1.at[i, jx, :, 0:width],
            send_sem=g1_s.at[0], recv_sem=g1_r.at[i],
            device_id=other, device_id_type=MESH)

    def gx_copy(i, jx):
        width = parts[i][1]
        return pltpu.make_async_remote_copy(
            src_ref=sx.at[i, jx - 1, :, 0:width], dst_ref=rx.at[i, jx - 1, :, 0:width],
            send_sem=gx_s.at[0], recv_sem=gx_r.at[i],
            device_id=(2 * lax.rem(x + jx, nx) + core, mv), device_id_type=MESH)

    def g2_copy(run):
        i, b, m, at, to, width = run
        return pltpu.make_async_remote_copy(
            src_ref=s2.at[i, :, at:at + width], dst_ref=r2.at[b * q + mm, :, to:to + width],
            send_sem=g2_s.at[0], recv_sem=g2_r.at[0],
            device_id=(d, pair_of(b) * q + m), device_id_type=MESH)

    def rz_copy(i):
        return pltpu.make_async_remote_copy(
            src_ref=s2.at[i, :, 0:span], dst_ref=rz,
            send_sem=rz_s.at[0], recv_sem=rz_r.at[0],
            device_id=(d, lax.rem(mg + nblk - 1, nblk) * q + mm), device_id_type=MESH)

    def gb_copy(run, jx):
        i, b, m, at, to, width = run
        return pltpu.make_async_remote_copy(
            src_ref=sb.at[i, jx, :, at:at + width], dst_ref=rb.at[(jx * nblk + b) * q + mm, :, to:to + width],
            send_sem=gb_s.at[0], recv_sem=gb_r.at[0],
            device_id=(2 * lax.rem(x + jx, nx) + core, pair_of(b) * q + m), device_id_type=MESH)

    for b in range(nblk):
        l_piece(b).start()
    for i in range(3):
        small_in(i).start()

    barrier = pltpu.get_barrier_semaphore()
    near = [(lax.rem(d + j, ndp), mv) for j in range(1, ndp)]
    near += [(d, mg * q + lax.rem(mm + j, q)) for j in range(1, q)]
    near += [(d, lax.rem(mg + j, nblk) * q + mm) for j in sorted({1, nblk - 1} - {0, nblk})]
    rounds = 1 + (q > 1) + nblk // 2

    def tell(sem):
        for to in near:
            pl.semaphore_signal(sem, inc=1, device_id=to, device_id_type=MESH)

    def heard(k):
        pl.semaphore_wait(known.at[k], len(near))
        if k + 2 < rounds:
            tell(known.at[k + 1])

    tell(barrier)
    for lo, hi in pieces:
        w_piece(lo, hi).start()

    top_n = ids_in.shape[1]
    for i in range(3):
        small_in(i).wait()
    tp_all[block(d), 0:top_n] = ids_v[...].astype(jnp.float32)
    tp_all[block(d), top_n:2 * top_n] = probs_v[...]
    drain(h_all.at[block(d), :], l_sem.at[0])
    pl.semaphore_wait(barrier, len(near))

    for j in range(1, nx):
        hx_copy(j, 0).start()
    tp_copy(other[0], True).start()
    for c in range(nk):
        hc_copy(0, c).start()
        if c > 0:
            for j in range(1, nx):
                hx_copy(j, c).start()
    for j in range(1, nx):
        for side in range(2):
            tp_copy(2 * lax.rem(x + j, nx) + side, False).start()

    if rounds > 1:
        tell(known.at[0])
    offset = (me * cols_n).astype(jnp.float32)
    nh = (cols_n + 255) // 256
    lane8 = lax.broadcasted_iota(jnp.int32, (8, 128), 1)
    sub8 = lax.broadcasted_iota(jnp.int32, (8, 128), 0)
    first8 = lane8 < top_n
    lo_iota = lax.broadcasted_iota(jnp.int32, (256, 128), 0)

    def build_group(t0):
        both = tp_all[pl.ds(t0, 8), :]
        turned = pltpu.roll(both, top_n, 1)
        ids = jnp.where(first8, both, turned)
        probs = jnp.where(first8, turned, both)
        high = probs.astype(jnp.bfloat16).astype(jnp.float32)
        rest = probs - high
        local = (ids - offset).astype(jnp.int32)
        inside = (local >= 0) & (local < cols_n)
        tile = jnp.where(inside, local >> 8, -1)
        low = local & 255
        left, right = [], []
        for u in range(4):
            tile_u = jnp.where(sub8 == jnp.where(first8, 2 * u, 2 * u + 1), tile, -1)
            left.append(jnp.concatenate(
                [jnp.where(tile_u == h, part, 0.0) for part in (high, rest) for h in range(nh)],
                axis=0).astype(jnp.bfloat16))
            low_u = jnp.where(first8[0:1], low[2 * u:2 * u + 1, :], low[2 * u + 1:2 * u + 2, :])
            right.append(jnp.where(lo_iota == low_u, 1.0, 0.0).astype(jnp.bfloat16))
        out = lax.dot_general(
            jnp.concatenate(left, axis=1), jnp.concatenate(right, axis=1), NT,
            preferred_element_type=jnp.float32)
        for h in range(nh):
            sp[pl.ds(t0, 8), h * 256:(h + 1) * 256] = (
                out[h * 8:(h + 1) * 8, :] + out[(nh + h) * 8:(nh + h + 1) * 8, :])
        mass = jnp.sum(jnp.where(first8, 0.0, both), axis=1, keepdims=True)
        cols[pl.ds(t0, 8), :] = jnp.broadcast_to(jnp.log(mass), (8, 128))

    deal = 4

    def build_block(dp_index):
        def build(step, _):
            for r in range(deal):
                build_group(pl.multiple_of(dp_index * rows + step * 8 * deal + 8 * r, 8))
            return 0

        lax.fori_loop(0, rows // (8 * deal), build, 0)

    build_block(d)
    drain(tp_all.at[block(d), :], tp_r.at[0])
    build_block(other[0])
    lt[(nt - 1) * 128:, :] = jnp.full((128, tok), -1e30, jnp.float32)

    def forward_in(c):
        first, width = parts[c]
        drain(h_all.at[0:(nx - 1) * rows, kpart(c)], hx_r.at[c])
        for j in range(1, nx):
            hc_copy(j, c).start()

    forward_in(0)
    halves = 2 * ((cols_n + 1023) // 1024)
    wide = ((cols_n + halves - 1) // halves + 15) // 16 * 16
    top = jnp.full((8, tok), -3e38, jnp.float32)
    turned_tiles = 0
    for c in range(nk):
        if c >= 4 and c % 2 == 0 and (c - 4) // 2 < rounds - 1:
            heard((c - 4) // 2)
        if c + 1 < nk:
            forward_in(c + 1)
        drain(h_all.at[0:nx * rows, kpart(c)], hc_r.at[c])
        drain(wv.at[:, kpart(c)], w_sem.at[c])
        hc = h_all[:, kpart(c)]
        for n0 in range(0, cols_n, wide):
            n1 = min(n0 + wide, cols_n)
            new = lax.dot_general(
                wv[n0:n1, kpart(c)], hc, NT, preferred_element_type=jnp.float32)
            if c == 0:
                lt[n0:n1, :] = new
            else:
                lt[n0:n1, :] += new
            if c == nk - 1:
                ready = nt if n1 == cols_n else n0 // 128
                for a in range(turned_tiles, ready):
                    value = lt[a * 128:(a + 1) * 128, :]
                    logits[:, a * 128:(a + 1) * 128] = value.T
                    for r in range(16):
                        top = jnp.maximum(top, value[8 * r:8 * r + 8, :])
                turned_tiles = max(turned_tiles, ready)

    m = jnp.max(top, axis=0, keepdims=True)
    deep = next(k for k in (304, 160, 152, 80, 64, 32, 16, 8) if nt * 128 % k == 0)

    def expsum(step, total):
        n0 = pl.multiple_of(step * deep, 8)
        for r in range(deep // 8):
            total += jnp.exp(lt[pl.ds(n0 + 8 * r, 8), :] - m)
        return total

    total = lax.fori_loop(0, nt * 128 // deep, expsum, jnp.zeros((8, tok), jnp.float32))
    s = jnp.sum(total, axis=0, keepdims=True)

    for k in range(len([c for c in range(4, nk) if c % 2 == 0]), rounds - 1):
        heard(k)
    for j in range(nb):
        stats[me, j:j + 1, :] = m[:, j * 128:(j + 1) * 128]
        stats[me, nb + j:nb + j + 1, :] = s[:, j * 128:(j + 1) * 128]
    for j in range(1, nd):
        st_copy(j, me).start()
    drain(tp_all.at[0:(ndp - 2) * rows, :], tp_r.at[1])
    for j in range(1, nx):
        for side in range(2):
            build_block(2 * lax.rem(x + j, nx) + side)
    back[...] = jnp.zeros_like(back)

    drain(stats.at[0:nd - 1, 0:2 * nb], st_r.at[0])
    for j in range(nb):
        part = slice(j * 128, (j + 1) * 128)
        ms = stats[:, j, :]
        big = jnp.max(ms, axis=0, keepdims=True)
        z = jnp.sum(stats[:, nb + j, :] * jnp.exp(ms - big), axis=0, keepdims=True)
        back[0:1, part] = big + jnp.log(z)
    cols2[...] = back[...].T


    def grad(step, _):
        t0 = pl.multiple_of(step * 16, 16)
        ts = pl.ds(t0, 16)
        shift = cols2[ts, 0:1] - cols[ts, 0:1]
        picked = jnp.zeros((16, 128), jnp.float32)
        for a in range(nt):
            n1 = min(128, cols_n - a * 128)
            value = logits[ts, a * 128:(a + 1) * 128]
            sparse = sp[ts, a * 128:(a + 1) * 128]
            picked += value * sparse
            lg[ts, a * 128:a * 128 + n1] = (
                jnp.exp(value - shift) - sparse)[:, :n1].astype(jnp.bfloat16)
        cols[ts, :] = picked
        return 0

    lax.fori_loop(0, tok // 16, grad, 0, unroll=2)

    def waits(run):
        return passed and run[1] == 2 and parts[run[0]][0] + run[3] < 2 * group + span

    def pair_sum(i, jx):
        mine_rows, width = block(2 * lax.rem(x + jx, nx) + core), parts[i][1]
        return g[i, mine_rows, 0:width] + r1[i, jx, :, 0:width]

    def to_x(i):
        width = parts[i][1]
        drain(r1.at[i, :, :, 0:width], g1_r.at[i])
        if direct[i]:
            for jx in list(range(1, nx)) + [0]:
                both = pair_sum(i, jx)
                sb[i, jx, :, 0:width] = both.astype(jnp.bfloat16)
                for run in late:
                    _, b, m, at, to, wide = run
                    if run[0] != i or (jx == 0 and waits(run)):
                        continue
                    if jx == 0 and b == nblk - 1:
                        @pl.when(m == mm)
                        def _():
                            own[:, to:to + wide] = both[:, at:at + wide]

                        pl.when(m != mm)(gb_copy(run, jx).start)
                    else:
                        gb_copy(run, jx).start()
            return
        for jx in range(1, nx):
            sx[i, jx - 1, :, 0:width] = pair_sum(i, jx).astype(jnp.bfloat16)
            gx_copy(i, jx).start()

    def to_vocab(i):
        if direct[i]:
            return
        width = parts[i][1]
        both = pair_sum(i, 0)
        drain(rx.at[i, :, :, 0:width], gx_r.at[i])
        for jx in range(1, nx):
            both += rx[i, jx - 1, :, 0:width].astype(jnp.float32)
        s2[i, :, 0:width] = both.astype(jnp.bfloat16)
        if passed and i == 0:
            rz_copy(i).start()
        for run in early:
            _, b, m, at, to, wide = run
            if run[0] != i:
                continue
            if b == nblk - 1:
                @pl.when(m == mm)
                def _():
                    own[:, to:to + wide] = both[:, at:at + wide]

                pl.when(m != mm)(g2_copy(run).start)
            else:
                g2_copy(run).start()

    lag = 3
    for i in range(ng):
        first, width = parts[i]
        g[i, :, 0:width] = jnp.dot(
            lg[...], wv[:, first:first + width], preferred_element_type=jnp.float32)
        for jx in range(nx):
            g1_copy(i, jx).start()
        if i == 0:
            turned = jnp.sum(cols[...].T, axis=0, keepdims=True)
            for j in range(nb):
                picks[me, j:j + 1, :] = turned[:, j * 128:(j + 1) * 128]
            for j in range(1, nd):
                pk_copy(j, me).start()
        if i >= 1:
            to_x(i - 1)
        if i >= lag:
            to_vocab(i - lag)
    to_x(ng - 1)
    for i in range(max(ng - lag, 0), ng):
        to_vocab(i)

    if passed:
        drain(rz, rz_r.at[0])
        for i in range(ng):
            first, width = parts[i]
            lo, hi = max(first, 2 * group), min(first + width, 2 * group + span)
            if lo < hi:
                mine_rows, at = block(2 * x + core), lo - 2 * group
                lo, hi = lo - first, hi - first
                sb[i, 0, :, lo:hi] = (
                    g[i, mine_rows, lo:hi] + r1[i, 0, :, lo:hi]
                    + rz[:, at:at + hi - lo].astype(jnp.float32)).astype(jnp.bfloat16)
            for run in late:
                if run[0] == i and waits(run):
                    gb_copy(run, 0).start()

    drain(picks.at[0:nd - 1, 0:nb], pk_r.at[0])
    for j in range(nb):
        back[1:2, j * 128:(j + 1) * 128] = jnp.sum(picks[:, j, :], axis=0, keepdims=True)
    cols2[...] = back[...].T
    mine = block(d)
    lane = lax.broadcasted_iota(jnp.int32, (rows, 128), 1)
    probs = jnp.where(lane >= top_n, tp_all[mine, :], 1.0)
    entropy = jnp.sum(probs * jnp.log(probs), axis=1, keepdims=True)
    mass = jnp.sum(jnp.where(lane >= top_n, probs, 0.0), axis=1, keepdims=True)
    diagonal = lax.broadcasted_iota(jnp.int32, (rows, rows), 0) == (
        lax.broadcasted_iota(jnp.int32, (rows, rows), 1))
    column = entropy - cols2[mine, 1:2] + mass * cols2[mine, 0:1]
    div_out[...] = jnp.sum(jnp.where(diagonal, column, 0.0), axis=0, keepdims=True)
    weight = jnp.sum(jnp.where(diagonal, tw_v[...], 0.0), axis=1, keepdims=True)

    for m in range(q):
        @pl.when(m == mm)
        def _():
            def arrivals(some, senders):
                return [(run, s) for run in some if run[2] == m for s in senders
                        if run[1] < nblk - 1 or s != m]

            def width_of(some):
                return sum(run[5] for run, _ in some)

            near = arrivals(early, range(q))
            if near:
                drain(strip(width_of(near)), g2_r.at[0])
            for (_, b, _, _, to, width), s in near:
                own[:, to:to + width] += r2[b * q + s, :, to:to + width].astype(jnp.float32)
            far = [(run, (jx * nblk + run[1]) * q + s)
                   for run in late if run[2] == m for jx in range(nx) for s in range(q)
                   if jx > 0 or run[1] < nblk - 1 or s != m]
            if far:
                drain(strip(width_of(far)), gb_r.at[0])
            for (_, b, _, _, to, width), s in far:
                own[:, to:to + width] += rb[s, :, to:to + width].astype(jnp.float32)
            lo = m * feat - starts[m]
            grad_out[...] = own[:, lo:lo + feat] * weight
            sent = sum(run[5] for run in early if run[1] < nblk - 1 or run[2] != m)
            if sent:
                drain(strip(sent), g2_s.at[0])
            sent = sum(run[5] for run in late for jx in range(nx)
                       if jx > 0 or run[1] < nblk - 1 or run[2] != m)
            if late:
                drain(strip(sent), gb_s.at[0])

    drain(h_all.at[0:(nx - 1) * rows, :], hx_s.at[0])
    drain(h_all.at[0:nx * rows, :], hc_s.at[0])
    drain(tp_all.at[0:(ndp - 1) * rows, :], tp_s.at[0])
    drain(stats.at[0:nd - 1, 0:2 * nb], st_s.at[0])
    if passed:
        drain(rz, rz_s.at[0])
    drain(picks.at[0:nd - 1, 0:nb], pk_s.at[0])
    drain(g.at[0:depth // g.shape[2], 0:nx * rows, :], g1_s.at[0])
    drain(strip((nx - 1) * sum(p[1] for p, far in zip(parts, direct) if not far)), gx_s.at[0])


def body(ndp, nv, hidden, head_weight, teacher_ids, teacher_probs, token_weight):
    rows, depth = hidden.shape
    cols_n = head_weight.shape[1]
    tok, nx, nd, feat = rows * ndp, ndp // 2, ndp * nv, depth // nv
    q, ww, _ = windows(feat)
    gw = max(width for _, width in spans(depth))
    nk = ng = len(spans(depth))
    nt = (cols_n + 127) // 128
    nh = (cols_n + 255) // 256
    srows = (2 * (tok // 128) + 7) // 8 * 8
    prows = (tok // 128 + 7) // 8 * 8
    f32, bf16, dma = jnp.float32, jnp.bfloat16, pltpu.SemaphoreType.DMA
    anyspace = pl.BlockSpec(memory_space=pl.ANY)
    vmem = pl.BlockSpec(memory_space=pltpu.VMEM)
    div, out = pl.pallas_call(
        functools.partial(kernel, ndp, nv),
        out_shape=(
            pltpu.VMEM((1, rows), f32), pltpu.VMEM((rows, feat), f32)),
        in_specs=[anyspace] * 5,
        out_specs=(vmem, vmem),
        scratch_shapes=[
            pltpu.VMEM((cols_n, depth), bf16), pltpu.VMEM((tok, depth), bf16),
            pltpu.VMEM(teacher_ids.shape, jnp.int32), pltpu.VMEM(teacher_probs.shape, f32),
            pltpu.VMEM((1, rows), f32),
            pltpu.VMEM((tok, 128), f32), pltpu.VMEM((tok, nh * 256), f32),
            pltpu.VMEM((nt * 128, tok), f32),
            pltpu.VMEM((tok, nt * 128), f32), pltpu.VMEM((tok, cols_n), bf16),
            pltpu.VMEM((ng, tok, gw), f32), pltpu.VMEM((ng, nx, rows, gw), f32),
            pltpu.VMEM((ng, nx - 1, rows, gw), bf16),
            pltpu.VMEM((ng, nx - 1, rows, gw), bf16),
            pltpu.VMEM((ng, rows, gw), bf16), pltpu.VMEM((nv, rows, ww), bf16),
            pltpu.VMEM((ng, nx, rows, gw), bf16), pltpu.VMEM((nx * nv, rows, ww), bf16), pltpu.VMEM((rows, gw), bf16),
            pltpu.VMEM((nd, srows, 128), f32), pltpu.VMEM((nd, prows, 128), f32),
            pltpu.VMEM((tok, 128), f32), pltpu.VMEM((tok, 128), f32),
            pltpu.VMEM((128, tok), f32), pltpu.VMEM((rows, ww), f32),
            dma((nk,)), dma((1,)), dma((3,)), dma((1,)), dma((1,)),
            dma((1,)), dma((nk,)), dma((1,)), dma((nk,)), dma((1,)), dma((2,)),
            dma((1,)), dma((1,)), dma((1,)), dma((ng,)), dma((1,)), dma((ng,)),
            dma((1,)), dma((1,)), dma((1,)), dma((1,)), dma((1,)), dma((1,)),
            pltpu.SemaphoreType.REGULAR((8,)),
        ],
        compiler_params=pltpu.CompilerParams(
            collective_id=0, has_side_effects=True, vmem_limit_bytes=66600000),
    )(hidden, head_weight.T, teacher_ids, teacher_probs, token_weight[None, :])
    return div[0], out


def solution(mesh):
    in_specs = (P("dp", None), P(None, ("dp", "vocab")), P("dp", None), P("dp", None), P("dp"))
    out_specs = (P("dp"), P("dp", "vocab"))
    return jax.shard_map(
        functools.partial(body, mesh.shape["dp"], mesh.shape["vocab"]),
        mesh=mesh, in_specs=in_specs, out_specs=out_specs, check_vma=False)
```

```python
import functools

import jax
import jax.numpy as jnp
from jax import lax
from jax.experimental import pallas as pl
from jax.experimental.pallas import tpu as pltpu
from jax.sharding import PartitionSpec as P

MESH = pl.DeviceIdType.MESH
NT = (((1,), (1,)), ((), ()))


def windows(feat):
    q = next(k for k in (1, 2, 4, 8, 16, 32, 64, 128) if k * feat % 128 == 0)
    first = [m * feat // 128 * 128 for m in range(q)]
    ww = max((m + 1) * feat - first[m] + 127 for m in range(q)) // 128 * 128
    return q, ww, [min(f, q * feat - ww) for f in first]


def spans(depth):
    wide = next(k for k in (512, 256, 128) if depth % k == 0)
    return [(first, wide) for first in range(0, depth, wide)]


def runs_of(depth, feat):
    q, ww, starts = windows(feat)
    out = []
    for b in range(depth // (q * feat)):
        for m in range(q):
            a = b * q * feat + starts[m]
            for i, (first, width) in enumerate(spans(depth)):
                lo, hi = max(a, first), min(a + ww, first + width)
                if lo < hi:
                    out.append((i, b, m, lo - first, lo - a, hi - lo))
    return out


def kernel(
    ndp, nv, hid, w, ids_in, probs_in, tw, div_out, grad_out,
    wv, h_all, ids_v, probs_v, tw_v, tp_all, sp, lt, logits, lg, g, r1, sx, rx, s2, r2, sb, rb, rz,
    stats, picks, cols, cols2, back, own,
    w_sem, l_sem, i_sem, pk_s, pk_r, hx_s, hx_r, hc_s, hc_r, tp_s, tp_r, st_s, st_r,
    g1_s, g1_r, gx_s, gx_r, g2_s, g2_r, gb_s, gb_r, rz_s, rz_r, known,
):
    d, mv = lax.axis_index("dp"), lax.axis_index("vocab")
    x, core = d // 2, d % 2
    nx, nd = ndp // 2, ndp * nv
    me = d * nv + mv
    rows, depth = hid.shape
    cols_n = w.shape[0]
    tok = rows * ndp
    parts = spans(depth)
    nk = ng = len(parts)
    nt = (cols_n + 127) // 128
    nb = tok // 128
    feat = depth // nv
    q, ww, starts = windows(feat)
    nblk, group = nv // q, q * feat
    runs = runs_of(depth, feat)
    direct = [i >= ng - 2 for i in range(ng)]
    shift = sorted(range(nblk), key=lambda o: (-min(o, nblk - o), o))
    span = parts[0][1]
    passed = nblk == 4 and span <= group and 3 * span <= 2 * group and (
        parts[ng - 2][0] >= 2 * group + span)
    early = [run for run in runs if not direct[run[0]] and not (passed and run[0] == 0)]
    late = [run for run in runs if direct[run[0]]]
    mg, mm = mv // q, lax.rem(mv, q)
    other = (2 * x + 1 - core, mv)

    def block(dp_index):
        return pl.ds(pl.multiple_of(dp_index * rows, rows), rows)

    def drain(ref, sem):
        pltpu.make_async_copy(ref, ref, sem).wait()

    def strip(width):
        units = rows * width // (8 * 128)
        tall = next(k for k in range(1, cols_n // 8 + 1)
                    if units % k == 0 and units // k <= depth // 128)
        return wv.at[0:tall * 8, 0:units // tall * 128]

    cuts = sorted({first for first, _ in parts} | set(range(0, depth, group)) | {depth})
    pieces = list(zip(cuts[:-1], cuts[1:]))

    def pair_of(b):
        return lax.rem(mg + shift[b], nblk)

    def source(lo, hi):
        begin = pair_of(lo // group) * group + lo % group
        return pl.ds(pl.multiple_of(begin, 128), hi - lo)

    def kpart(c):
        return pl.ds(*parts[c])

    def w_piece(lo, hi):
        c = max(c for c in range(nk) if parts[c][0] <= lo)
        return pltpu.make_async_copy(
            w.at[:, source(lo, hi)], wv.at[:, lo:hi], w_sem.at[c])

    def l_piece(b):
        lo, hi = b * group, (b + 1) * group
        return pltpu.make_async_copy(
            hid.at[:, source(lo, hi)], h_all.at[block(d), lo:hi], l_sem.at[0])

    def hx_copy(j, c):
        return pltpu.make_async_remote_copy(
            src_ref=h_all.at[block(d), kpart(c)], dst_ref=h_all.at[block(d), kpart(c)],
            send_sem=hx_s.at[0], recv_sem=hx_r.at[c],
            device_id=(2 * lax.rem(x + j, nx) + core, mv), device_id_type=MESH)

    def hc_copy(j, c):
        src = h_all.at[block(2 * lax.rem(x + nx - j, nx) + core), kpart(c)]
        return pltpu.make_async_remote_copy(
            src_ref=src, dst_ref=src,
            send_sem=hc_s.at[0], recv_sem=hc_r.at[c],
            device_id=other, device_id_type=MESH)

    def tp_copy(to, near):
        return pltpu.make_async_remote_copy(
            src_ref=tp_all.at[block(d), :], dst_ref=tp_all.at[block(d), :],
            send_sem=tp_s.at[0], recv_sem=tp_r.at[0 if near else 1],
            device_id=(to, mv), device_id_type=MESH)

    def st_copy(j, sender):
        to = lax.rem(me + j, nd)
        return pltpu.make_async_remote_copy(
            src_ref=stats.at[sender, 0:2 * nb], dst_ref=stats.at[sender, 0:2 * nb],
            send_sem=st_s.at[0], recv_sem=st_r.at[0],
            device_id=(to // nv, lax.rem(to, nv)), device_id_type=MESH)

    def pk_copy(j, sender):
        to = lax.rem(me + j, nd)
        return pltpu.make_async_remote_copy(
            src_ref=picks.at[sender, 0:nb], dst_ref=picks.at[sender, 0:nb],
            send_sem=pk_s.at[0], recv_sem=pk_r.at[0],
            device_id=(to // nv, lax.rem(to, nv)), device_id_type=MESH)

    def small_in(i):
        src, dst = ((ids_in, ids_v), (probs_in, probs_v), (tw, tw_v))[i]
        return pltpu.make_async_copy(src, dst, i_sem.at[i])

    def g1_copy(i, jx):
        theirs = block(2 * lax.rem(x + jx, nx) + 1 - core)
        width = parts[i][1]
        return pltpu.make_async_remote_copy(
            src_ref=g.at[i, theirs, 0:width], dst_ref=r1.at[i, jx, :, 0:width],
            send_sem=g1_s.at[0], recv_sem=g1_r.at[i],
            device_id=other, device_id_type=MESH)

    def gx_copy(i, jx):
        width = parts[i][1]
        return pltpu.make_async_remote_copy(
            src_ref=sx.at[i, jx - 1, :, 0:width], dst_ref=rx.at[i, jx - 1, :, 0:width],
            send_sem=gx_s.at[0], recv_sem=gx_r.at[i],
            device_id=(2 * lax.rem(x + jx, nx) + core, mv), device_id_type=MESH)

    def g2_copy(run):
        i, b, m, at, to, width = run
        return pltpu.make_async_remote_copy(
            src_ref=s2.at[i, :, at:at + width], dst_ref=r2.at[b * q + mm, :, to:to + width],
            send_sem=g2_s.at[0], recv_sem=g2_r.at[0],
            device_id=(d, pair_of(b) * q + m), device_id_type=MESH)

    def rz_copy(i):
        return pltpu.make_async_remote_copy(
            src_ref=s2.at[i, :, 0:span], dst_ref=rz,
            send_sem=rz_s.at[0], recv_sem=rz_r.at[0],
            device_id=(d, lax.rem(mg + nblk - 1, nblk) * q + mm), device_id_type=MESH)

    def gb_copy(run, jx):
        i, b, m, at, to, width = run
        return pltpu.make_async_remote_copy(
            src_ref=sb.at[i, jx, :, at:at + width], dst_ref=rb.at[(jx * nblk + b) * q + mm, :, to:to + width],
            send_sem=gb_s.at[0], recv_sem=gb_r.at[0],
            device_id=(2 * lax.rem(x + jx, nx) + core, pair_of(b) * q + m), device_id_type=MESH)

    for b in range(nblk):
        l_piece(b).start()
    for i in range(3):
        small_in(i).start()

    barrier = pltpu.get_barrier_semaphore()
    near = [(lax.rem(d + j, ndp), mv) for j in range(1, ndp)]
    near += [(d, mg * q + lax.rem(mm + j, q)) for j in range(1, q)]
    near += [(d, lax.rem(mg + j, nblk) * q + mm) for j in sorted({1, nblk - 1} - {0, nblk})]
    rounds = 1 + (q > 1) + nblk // 2

    def tell(sem):
        for to in near:
            pl.semaphore_signal(sem, inc=1, device_id=to, device_id_type=MESH)

    def heard(k):
        pl.semaphore_wait(known.at[k], len(near))
        if k + 2 < rounds:
            tell(known.at[k + 1])

    tell(barrier)
    for lo, hi in pieces:
        w_piece(lo, hi).start()

    top_n = ids_in.shape[1]
    for i in range(3):
        small_in(i).wait()
    tp_all[block(d), 0:top_n] = ids_v[...].astype(jnp.float32)
    tp_all[block(d), top_n:2 * top_n] = probs_v[...]
    drain(h_all.at[block(d), :], l_sem.at[0])
    pl.semaphore_wait(barrier, len(near))

    for j in range(1, nx):
        hx_copy(j, 0).start()
    tp_copy(other[0], True).start()
    for c in range(nk):
        hc_copy(0, c).start()
        if c > 0:
            for j in range(1, nx):
                hx_copy(j, c).start()
    for j in range(1, nx):
        for side in range(2):
            tp_copy(2 * lax.rem(x + j, nx) + side, False).start()

    if rounds > 1:
        tell(known.at[0])
    offset = (me * cols_n).astype(jnp.float32)
    nh = (cols_n + 255) // 256
    lane8 = lax.broadcasted_iota(jnp.int32, (8, 128), 1)
    sub8 = lax.broadcasted_iota(jnp.int32, (8, 128), 0)
    first8 = lane8 < top_n
    lo_iota = lax.broadcasted_iota(jnp.int32, (256, 128), 0)

    def build_group(t0):
        both = tp_all[pl.ds(t0, 8), :]
        turned = pltpu.roll(both, top_n, 1)
        ids = jnp.where(first8, both, turned)
        probs = jnp.where(first8, turned, both)
        high = probs.astype(jnp.bfloat16).astype(jnp.float32)
        rest = probs - high
        local = (ids - offset).astype(jnp.int32)
        inside = (local >= 0) & (local < cols_n)
        tile = jnp.where(inside, local >> 8, -1)
        low = local & 255
        left, right = [], []
        for u in range(4):
            tile_u = jnp.where(sub8 == jnp.where(first8, 2 * u, 2 * u + 1), tile, -1)
            left.append(jnp.concatenate(
                [jnp.where(tile_u == h, part, 0.0) for part in (high, rest) for h in range(nh)],
                axis=0).astype(jnp.bfloat16))
            low_u = jnp.where(first8[0:1], low[2 * u:2 * u + 1, :], low[2 * u + 1:2 * u + 2, :])
            right.append(jnp.where(lo_iota == low_u, 1.0, 0.0).astype(jnp.bfloat16))
        out = lax.dot_general(
            jnp.concatenate(left, axis=1), jnp.concatenate(right, axis=1), NT,
            preferred_element_type=jnp.float32)
        for h in range(nh):
            sp[pl.ds(t0, 8), h * 256:(h + 1) * 256] = (
                out[h * 8:(h + 1) * 8, :] + out[(nh + h) * 8:(nh + h + 1) * 8, :])
        mass = jnp.sum(jnp.where(first8, 0.0, both), axis=1, keepdims=True)
        cols[pl.ds(t0, 8), :] = jnp.broadcast_to(jnp.log(mass), (8, 128))

    deal = 4

    def build_block(dp_index):
        def build(step, _):
            for r in range(deal):
                build_group(pl.multiple_of(dp_index * rows + step * 8 * deal + 8 * r, 8))
            return 0

        lax.fori_loop(0, rows // (8 * deal), build, 0)

    build_block(d)
    drain(tp_all.at[block(d), :], tp_r.at[0])
    build_block(other[0])
    lt[(nt - 1) * 128:, :] = jnp.full((128, tok), -1e30, jnp.float32)

    def forward_in(c):
        first, width = parts[c]
        drain(h_all.at[0:(nx - 1) * rows, kpart(c)], hx_r.at[c])
        for j in range(1, nx):
            hc_copy(j, c).start()

    forward_in(0)
    halves = 2 * ((cols_n + 1023) // 1024)
    wide = ((cols_n + halves - 1) // halves + 15) // 16 * 16
    top = jnp.full((8, tok), -3e38, jnp.float32)
    turned_tiles = 0
    for c in range(nk):
        if c >= 4 and c % 2 == 0 and (c - 4) // 2 < rounds - 1:
            heard((c - 4) // 2)
        if c + 1 < nk:
            forward_in(c + 1)
        drain(h_all.at[0:nx * rows, kpart(c)], hc_r.at[c])
        drain(wv.at[:, kpart(c)], w_sem.at[c])
        hc = h_all[:, kpart(c)]
        for n0 in range(0, cols_n, wide):
            n1 = min(n0 + wide, cols_n)
            new = lax.dot_general(
                wv[n0:n1, kpart(c)], hc, NT, preferred_element_type=jnp.float32)
            if c == 0:
                lt[n0:n1, :] = new
            else:
                lt[n0:n1, :] += new
            if c == nk - 1:
                ready = nt if n1 == cols_n else n0 // 128
                for a in range(turned_tiles, ready):
                    value = lt[a * 128:(a + 1) * 128, :]
                    logits[:, a * 128:(a + 1) * 128] = value.T
                    for r in range(16):
                        top = jnp.maximum(top, value[8 * r:8 * r + 8, :])
                turned_tiles = max(turned_tiles, ready)

    m = jnp.max(top, axis=0, keepdims=True)
    deep = next(k for k in (304, 160, 152, 80, 64, 32, 16, 8) if nt * 128 % k == 0)

    def expsum(step, total):
        n0 = pl.multiple_of(step * deep, 8)
        for r in range(deep // 8):
            total += jnp.exp(lt[pl.ds(n0 + 8 * r, 8), :] - m)
        return total

    total = lax.fori_loop(0, nt * 128 // deep, expsum, jnp.zeros((8, tok), jnp.float32))
    s = jnp.sum(total, axis=0, keepdims=True)

    for k in range(len([c for c in range(4, nk) if c % 2 == 0]), rounds - 1):
        heard(k)
    for j in range(nb):
        stats[me, j:j + 1, :] = m[:, j * 128:(j + 1) * 128]
        stats[me, nb + j:nb + j + 1, :] = s[:, j * 128:(j + 1) * 128]
    for j in range(1, nd):
        st_copy(j, me).start()
    drain(tp_all.at[0:(ndp - 2) * rows, :], tp_r.at[1])
    for j in range(1, nx):
        for side in range(2):
            build_block(2 * lax.rem(x + j, nx) + side)
    back[...] = jnp.zeros_like(back)

    drain(stats.at[0:nd - 1, 0:2 * nb], st_r.at[0])
    for j in range(nb):
        part = slice(j * 128, (j + 1) * 128)
        ms = stats[:, j, :]
        big = jnp.max(ms, axis=0, keepdims=True)
        z = jnp.sum(stats[:, nb + j, :] * jnp.exp(ms - big), axis=0, keepdims=True)
        back[0:1, part] = big + jnp.log(z)
    cols2[...] = back[...].T


    def grad(step, _):
        t0 = pl.multiple_of(step * 16, 16)
        ts = pl.ds(t0, 16)
        shift = cols2[ts, 0:1] - cols[ts, 0:1]
        picked = jnp.zeros((16, 128), jnp.float32)
        for a in range(nt):
            n1 = min(128, cols_n - a * 128)
            value = logits[ts, a * 128:(a + 1) * 128]
            sparse = sp[ts, a * 128:(a + 1) * 128]
            picked += value * sparse
            lg[ts, a * 128:a * 128 + n1] = (
                jnp.exp(value - shift) - sparse)[:, :n1].astype(jnp.bfloat16)
        cols[ts, :] = picked
        return 0

    lax.fori_loop(0, tok // 16, grad, 0, unroll=2)

    def pair_sum(i, jx):
        mine_rows, width = block(2 * lax.rem(x + jx, nx) + core), parts[i][1]
        return g[i, mine_rows, 0:width] + r1[i, jx, :, 0:width]

    def to_x(i):
        width = parts[i][1]
        drain(r1.at[i, :, :, 0:width], g1_r.at[i])
        if direct[i]:
            for jx in list(range(1, nx)) + [0]:
                both = pair_sum(i, jx)
                sb[i, jx, :, 0:width] = both.astype(jnp.bfloat16)
                for run in late:
                    _, b, m, at, to, wide = run
                    if run[0] != i:
                        continue
                    if jx == 0 and b == nblk - 1:
                        @pl.when(m == mm)
                        def _():
                            own[:, to:to + wide] = both[:, at:at + wide]

                        pl.when(m != mm)(gb_copy(run, jx).start)
                    else:
                        gb_copy(run, jx).start()
            return
        for jx in range(1, nx):
            sx[i, jx - 1, :, 0:width] = pair_sum(i, jx).astype(jnp.bfloat16)
            gx_copy(i, jx).start()

    def to_vocab(i):
        if direct[i]:
            return
        first, width = parts[i]
        both = pair_sum(i, 0)
        drain(rx.at[i, :, :, 0:width], gx_r.at[i])
        for jx in range(1, nx):
            both += rx[i, jx - 1, :, 0:width].astype(jnp.float32)
        if passed:
            lo, hi = max(first, 2 * group), min(first + width, 2 * group + span)
            if lo < hi:
                added = rz[:, lo - 2 * group:hi - 2 * group].astype(jnp.float32)
                pad = [jnp.zeros((rows, n), jnp.float32) for n in (lo - first, first + width - hi)]
                both += jnp.concatenate(
                    [p for p in (pad[0], added, pad[1]) if p.shape[1] > 0], axis=1)
        s2[i, :, 0:width] = both.astype(jnp.bfloat16)
        if passed and i == 0:
            rz_copy(i).start()
        for run in early:
            _, b, m, at, to, wide = run
            if run[0] != i:
                continue
            if b == nblk - 1:
                @pl.when(m == mm)
                def _():
                    own[:, to:to + wide] = both[:, at:at + wide]

                pl.when(m != mm)(g2_copy(run).start)
            else:
                g2_copy(run).start()

    lag, head = 3, 3 if passed else ng
    for i in range(ng):
        first, width = parts[i]
        g[i, :, 0:width] = jnp.dot(
            lg[...], wv[:, first:first + width], preferred_element_type=jnp.float32)
        for jx in range(nx):
            g1_copy(i, jx).start()
        if i >= 1:
            to_x(i - 1)
        if i == min(1, ng - 1):
            turned = jnp.sum(cols[...].T, axis=0, keepdims=True)
            for j in range(nb):
                picks[me, j:j + 1, :] = turned[:, j * 128:(j + 1) * 128]
            for j in range(1, nd):
                pk_copy(j, me).start()
        if lag <= i < lag + head:
            to_vocab(i - lag)
    rest = list(range(max(min(head, ng - lag), 0), ng))
    if passed:
        drain(rz, rz_r.at[0])
        to_vocab(rest.pop(0))
    to_x(ng - 1)
    for i in rest:
        to_vocab(i)

    drain(picks.at[0:nd - 1, 0:nb], pk_r.at[0])
    for j in range(nb):
        back[1:2, j * 128:(j + 1) * 128] = jnp.sum(picks[:, j, :], axis=0, keepdims=True)
    cols2[...] = back[...].T
    mine = block(d)
    lane = lax.broadcasted_iota(jnp.int32, (rows, 128), 1)
    probs = jnp.where(lane >= top_n, tp_all[mine, :], 1.0)
    entropy = jnp.sum(probs * jnp.log(probs), axis=1, keepdims=True)
    mass = jnp.sum(jnp.where(lane >= top_n, probs, 0.0), axis=1, keepdims=True)
    diagonal = lax.broadcasted_iota(jnp.int32, (rows, rows), 0) == (
        lax.broadcasted_iota(jnp.int32, (rows, rows), 1))
    column = entropy - cols2[mine, 1:2] + mass * cols2[mine, 0:1]
    div_out[...] = jnp.sum(jnp.where(diagonal, column, 0.0), axis=0, keepdims=True)
    weight = jnp.sum(jnp.where(diagonal, tw_v[...], 0.0), axis=1, keepdims=True)

    for m in range(q):
        @pl.when(m == mm)
        def _():
            def arrivals(some, senders):
                return [(run, s) for run in some if run[2] == m for s in senders
                        if run[1] < nblk - 1 or s != m]

            def width_of(some):
                return sum(run[5] for run, _ in some)

            near = arrivals(early, range(q))
            if near:
                drain(strip(width_of(near)), g2_r.at[0])
            for (_, b, _, _, to, width), s in near:
                own[:, to:to + width] += r2[b * q + s, :, to:to + width].astype(jnp.float32)
            far = [(run, (jx * nblk + run[1]) * q + s)
                   for run in late if run[2] == m for jx in range(nx) for s in range(q)
                   if jx > 0 or run[1] < nblk - 1 or s != m]
            if far:
                drain(strip(width_of(far)), gb_r.at[0])
            for (_, b, _, _, to, width), s in far:
                own[:, to:to + width] += rb[s, :, to:to + width].astype(jnp.float32)
            lo = m * feat - starts[m]
            grad_out[...] = own[:, lo:lo + feat] * weight
            sent = sum(run[5] for run in early if run[1] < nblk - 1 or run[2] != m)
            if sent:
                drain(strip(sent), g2_s.at[0])
            sent = sum(run[5] for run in late for jx in range(nx)
                       if jx > 0 or run[1] < nblk - 1 or run[2] != m)
            if late:
                drain(strip(sent), gb_s.at[0])

    drain(h_all.at[0:(nx - 1) * rows, :], hx_s.at[0])
    drain(h_all.at[0:nx * rows, :], hc_s.at[0])
    drain(tp_all.at[0:(ndp - 1) * rows, :], tp_s.at[0])
    drain(stats.at[0:nd - 1, 0:2 * nb], st_s.at[0])
    if passed:
        drain(rz, rz_s.at[0])
    drain(picks.at[0:nd - 1, 0:nb], pk_s.at[0])
    drain(g.at[0:depth // g.shape[2], 0:nx * rows, :], g1_s.at[0])
    drain(strip((nx - 1) * sum(p[1] for p, far in zip(parts, direct) if not far)), gx_s.at[0])


def body(ndp, nv, hidden, head_weight, teacher_ids, teacher_probs, token_weight):
    rows, depth = hidden.shape
    cols_n = head_weight.shape[1]
    tok, nx, nd, feat = rows * ndp, ndp // 2, ndp * nv, depth // nv
    q, ww, _ = windows(feat)
    gw = max(width for _, width in spans(depth))
    nk = ng = len(spans(depth))
    nt = (cols_n + 127) // 128
    nh = (cols_n + 255) // 256
    srows = (2 * (tok // 128) + 7) // 8 * 8
    prows = (tok // 128 + 7) // 8 * 8
    f32, bf16, dma = jnp.float32, jnp.bfloat16, pltpu.SemaphoreType.DMA
    anyspace = pl.BlockSpec(memory_space=pl.ANY)
    vmem = pl.BlockSpec(memory_space=pltpu.VMEM)
    div, out = pl.pallas_call(
        functools.partial(kernel, ndp, nv),
        out_shape=(
            pltpu.VMEM((1, rows), f32), pltpu.VMEM((rows, feat), f32)),
        in_specs=[anyspace] * 5,
        out_specs=(vmem, vmem),
        scratch_shapes=[
            pltpu.VMEM((cols_n, depth), bf16), pltpu.VMEM((tok, depth), bf16),
            pltpu.VMEM(teacher_ids.shape, jnp.int32), pltpu.VMEM(teacher_probs.shape, f32),
            pltpu.VMEM((1, rows), f32),
            pltpu.VMEM((tok, 128), f32), pltpu.VMEM((tok, nh * 256), f32),
            pltpu.VMEM((nt * 128, tok), f32),
            pltpu.VMEM((tok, nt * 128), f32), pltpu.VMEM((tok, cols_n), bf16),
            pltpu.VMEM((ng, tok, gw), f32), pltpu.VMEM((ng, nx, rows, gw), f32),
            pltpu.VMEM((ng, nx - 1, rows, gw), bf16),
            pltpu.VMEM((ng, nx - 1, rows, gw), bf16),
            pltpu.VMEM((ng, rows, gw), bf16), pltpu.VMEM((nv, rows, ww), bf16),
            pltpu.VMEM((ng, nx, rows, gw), bf16), pltpu.VMEM((nx * nv, rows, ww), bf16), pltpu.VMEM((rows, gw), bf16),
            pltpu.VMEM((nd, srows, 128), f32), pltpu.VMEM((nd, prows, 128), f32),
            pltpu.VMEM((tok, 128), f32), pltpu.VMEM((tok, 128), f32),
            pltpu.VMEM((128, tok), f32), pltpu.VMEM((rows, ww), f32),
            dma((nk,)), dma((1,)), dma((3,)), dma((1,)), dma((1,)),
            dma((1,)), dma((nk,)), dma((1,)), dma((nk,)), dma((1,)), dma((2,)),
            dma((1,)), dma((1,)), dma((1,)), dma((ng,)), dma((1,)), dma((ng,)),
            dma((1,)), dma((1,)), dma((1,)), dma((1,)), dma((1,)), dma((1,)),
            pltpu.SemaphoreType.REGULAR((8,)),
        ],
        compiler_params=pltpu.CompilerParams(
            collective_id=0, has_side_effects=True, vmem_limit_bytes=66600000),
    )(hidden, head_weight.T, teacher_ids, teacher_probs, token_weight[None, :])
    return div[0], out


def solution(mesh):
    in_specs = (P("dp", None), P(None, ("dp", "vocab")), P("dp", None), P("dp", None), P("dp"))
    out_specs = (P("dp"), P("dp", "vocab"))
    return jax.shard_map(
        functools.partial(body, mesh.shape["dp"], mesh.shape["vocab"]),
        mesh=mesh, in_specs=in_specs, out_specs=out_specs, check_vma=False)
```
